32 devices in a mesh: grp: 4 (over x, core), shard: 8 (over z, y).
Axes of the slice: x: 2, y: 2, z: 4, core: 2. Of those that a mesh axis runs over, the one named last changes fastest.
Arguments:
- inputs: bfloat16 [16384, 1024], P(('grp', 'shard')), may hold values from -6 to 6
- cotangent: bfloat16 [16384, 1024], P(('grp', 'shard')), may hold values from -6 to 6
- doc_ids: int32 [16384], P(('grp', 'shard')), may hold values from 0 to 1, as said below
- master_in: float32 [1024, 7168], P('shard'), may hold values from -0.1875 to 0.1875
- master_out: float32 [5120, 1024], P('shard'), may hold values from -6 to 6
- vectors: float32 [12, 1024], P(None, 'shard'), may hold values from -2 to 2, as said below
- moment_in: float32 [1024, 7168], P('shard'), may hold values from -24 to 24
- moment_out: float32 [5120, 1024], P('shard'), may hold values from -24 to 24
- moment_vec: float32 [12, 1024], P(None, 'shard'), may hold values from -24 to 24
- square_in: float32 [1024, 7168], P('shard'), may hold values from 4 to 1000
- square_out: float32 [5120, 1024], P('shard'), may hold values from 4 to 1000
- square_vec: float32 [12, 1024], P(None, 'shard'), may hold values from 4 to 1000
Outputs:
- output: bfloat16 [16384, 1024], P(('grp', 'shard'))
- input_grad: float32 [16384, 1024], P(('grp', 'shard'))
- grad_in: float32 [1024, 7168], P('shard')
- grad_out: float32 [5120, 1024], P('shard')
- grad_vec: float32 [12, 1024], P(None, 'shard')
- update_in: float32 [1024, 7168], P('shard')
- update_out: float32 [5120, 1024], P('shard')
- update_vec: float32 [12, 1024], P(None, 'shard')
- moment_in_next: float32 [1024, 7168], P('shard')
- moment_out_next: float32 [5120, 1024], P('shard')
- moment_vec_next: float32 [12, 1024], P(None, 'shard')
- square_in_next: float32 [1024, 7168], P('shard')
- square_out_next: float32 [5120, 1024], P('shard')
- square_vec_next: float32 [12, 1024], P(None, 'shard')
The draws below stay inside these ranges and needn't reach their ends.
Inputs may be any that keep to these rules, and one draw needn't show every extreme that they name: `doc_ids`: on each device the ids never fall along its 512 slots; each id j < 1 covers 8 to 512 slots in a row; id 1 covers the padding after them; on some device every sequence has 512 slots. `vectors`: rows 0 and 2 lie between 0.6 and 1.4.
All inputs are finite; a program needn't handle non-finite values.
Results may differ from the reference program's by a relative error of at most 0.035.
Values may be sent and summed in bfloat16 or wider, within the bound.
A program may use at most 320 MiB of HBM per device.

```python
import math
import jax
import jax.numpy as jnp
from jax import lax

D = 1024
HEAD = 64
FF = 4096
ROT = 16
MAXLEN = 512
SEQ_DEV = 1
STEP = 10
SLOTS = 512
TOKENS = 16384


def draw_doc_ids(key, part):
    devices = TOKENS // SLOTS
    key_len, key_dev = jax.random.split(key)
    lengths = jax.random.randint(key_len, (devices, SEQ_DEV), 8, MAXLEN + 1)
    full_device = jax.random.randint(key_dev, (), 0, devices)
    lengths = jnp.where(jnp.arange(devices)[:, None] == full_device, MAXLEN, lengths)
    ends = jnp.cumsum(lengths, axis=1)
    slot = jnp.arange(SLOTS)
    ids = jnp.sum((slot[None, :, None] >= ends[:, None, :]).astype(jnp.int32), axis=2)
    return ids.reshape(devices * SLOTS).astype(jnp.int32)


def draw_master_out(key, part):
    values = jnp.clip(jax.random.normal(key, (D + FF, D), jnp.float32), -6.0, 6.0)
    row = jnp.arange(D + FF)[:, None]
    scale = jnp.where(row < D, 8.0 / math.sqrt(D), 1.0 / math.sqrt(FF))
    return jnp.clip(values * scale, -6.0, 6.0)


def draw_vectors(key, part):
    key_shift, key_gain = jax.random.split(key)
    shifts = jnp.clip(jax.random.normal(key_shift, (12, D), jnp.float32), -4.0, 4.0)
    gains = jax.random.uniform(key_gain, (12, D), jnp.float32, 0.6, 1.4)
    row = jnp.arange(12)[:, None]
    spread = jnp.where(row < 4, 0.3, 0.5)
    return jnp.where((row == 0) | (row == 2), gains, shifts * spread)


def raised(values, own_key, source, target, shards_of, factor):
    owner, partner = [(jnp.arange(values.shape[dim]) // (values.shape[dim] // shards_of)).reshape([-1 if axis == dim else 1 for axis in range(values.ndim)]) for dim in (source, target)]
    chosen = jax.random.permutation(own_key, shards_of)[partner]
    strong = (owner == chosen) | (owner == (partner + shards_of // 2) % shards_of)
    return jnp.where(strong, factor * values, values)


def level_of(own_key, extent, cuts, low, largest):
    factor_of = 1.0
    for axis_at, blocks in cuts:
        steps = jax.random.uniform(jax.random.fold_in(jax.random.fold_in(own_key, 6), axis_at), (blocks,), jnp.float32, low / len(cuts), largest / len(cuts))
        factor_of = factor_of * jnp.repeat(jnp.exp(steps), extent[axis_at] // blocks).reshape((-1,) + (1,) * (len(extent) - 1 - axis_at))
    return factor_of


def gaussian(rng, extent, deviation, limit, cuts=(), kind=jnp.bfloat16):
    gain = level_of(rng, extent, cuts, -0.22, 0.18) if cuts else 1.0
    values = jax.random.normal(rng, extent, jnp.float32) * deviation * gain
    return jnp.minimum(jnp.maximum(values, -limit), limit).astype(kind)


def gaussian_with(rng, shape, deviation, bound, cuts, heavy, kind=jnp.bfloat16):
    entries = deviation * jax.random.normal(rng, shape, jnp.float32)
    if cuts:
        entries = entries * level_of(rng, shape, cuts, -0.22, 0.18)
    return jnp.clip(raised(entries, jax.random.fold_in(rng, 3), *heavy), -bound, bound).astype(kind)


def setup_inputs(seed: int = 0) -> dict:
    key_list = jax.random.split(jax.random.key(seed), 13)
    inputs = gaussian_with(key_list[0], (TOKENS, D), 1.0, 6.0, ((0, 32),), (0, 1, 32, 2.75))
    cotangent = gaussian(key_list[1], (TOKENS, D), 1.0, 6.0, ((0, 32),))
    doc_ids = draw_doc_ids(jax.random.fold_in(key_list[12], 71), 0)
    master_in = gaussian(key_list[3], (D, 3 * D + FF), D ** -0.5, 0.1875, ((0, 8),), jnp.float32)
    master_out = draw_master_out(jax.random.fold_in(key_list[12], 71), 0)
    vectors = draw_vectors(jax.random.fold_in(key_list[12], 71), 0)
    moment_in = gaussian(key_list[6], (D, 3 * D + FF), 4.0, 24.0, ((0, 8),), jnp.float32)
    moment_out = gaussian(key_list[7], (D + FF, D), 4.0, 24.0, ((0, 8),), jnp.float32)
    moment_vec = gaussian(key_list[8], (12, D), 4.0, 24.0, ((1, 8),), jnp.float32)
    square_in = jnp.clip(jnp.exp(math.log(1000.0) - 5.521461 * jax.random.uniform(key_list[9], (D, 3 * D + FF), jnp.float32) ** level_of(key_list[9], (D, 3 * D + FF), ((0, 8),), -0.2, 0.2)), 4.0, 1000.0)
    square_out = jnp.clip(jnp.exp(math.log(1000.0) - 5.521461 * jax.random.uniform(key_list[10], (D + FF, D), jnp.float32) ** level_of(key_list[10], (D + FF, D), ((0, 8),), -0.2, 0.2)), 4.0, 1000.0)
    square_vec = jnp.clip(jnp.exp(math.log(1000.0) - 5.521461 * jax.random.uniform(key_list[11], (12, D), jnp.float32) ** level_of(key_list[11], (12, D), ((1, 8),), -0.2, 0.2)), 4.0, 1000.0)
    return dict(inputs=inputs, cotangent=cotangent, doc_ids=doc_ids, master_in=master_in, master_out=master_out, vectors=vectors, moment_in=moment_in, moment_out=moment_out, moment_vec=moment_vec, square_in=square_in, square_out=square_out, square_vec=square_vec)


NEG = -1e+30
HIGH = lax.Precision.HIGHEST

@jax.custom_vjp
def low(v):
    return lax.optimization_barrier(v.astype(jnp.bfloat16)).astype(jnp.float32)

@jax.custom_vjp
def low_back(v):
    return v

def low_keep(v):
    return (low(v), None)

def low_pass(kept, grad):
    return (grad,)

def back_keep(v):
    return (v, None)

def back_low(kept, grad):
    return (low(grad),)
low.defvjp(low_keep, low_pass)
low_back.defvjp(back_keep, back_low)

def tables(doc):
    count = doc.shape[0]
    order = jnp.arange(count, dtype=jnp.int32)
    first = lax.optimization_barrier(jnp.sum((doc[None, :] < doc[:, None]).astype(jnp.int32), axis=1))
    position = (order - first).astype(jnp.float32)
    half = ROT // 2
    freq = 10000.0 ** (-(jnp.arange(half, dtype=jnp.float32) * 2.0 / ROT))
    angle = position[:, None] * freq[None, :]
    angle = jnp.concatenate([angle, angle], axis=1)
    return (jnp.cos(angle), jnp.sin(angle))

def rotate(values, cosine, sine):
    half = ROT // 2
    part = values[..., :ROT]
    turned = jnp.concatenate([-part[..., half:], part[..., :half]], axis=-1)
    moved = part * cosine[:, None, :] + turned * sine[:, None, :]
    return jnp.concatenate([moved, values[..., ROT:]], axis=-1)

def layer_norm(residual_stream, norm_gain, norm_offset):
    feature_mean = lax.optimization_barrier(jnp.mean(residual_stream, axis=-1, keepdims=True))
    mean_removed = residual_stream - feature_mean
    var = lax.optimization_barrier(jnp.mean(mean_removed * mean_removed, axis=-1, keepdims=True))
    return mean_removed * lax.rsqrt(var + 1e-05) * norm_gain + norm_offset

def forward(residual_stream, master_in, master_out, vectors, doc):
    w_in = low(master_in)
    w_out = low(master_out)
    packed = low(vectors)
    slots, width = residual_stream.shape
    heads = width // HEAD
    bias_qkv = packed[4:7].reshape(3 * width)
    bias_hidden = packed[7:11].reshape(4 * width)
    branch_input_first = low(layer_norm(residual_stream, packed[0], packed[1]))
    branch_input_second = low(layer_norm(residual_stream, packed[2], packed[3]))
    qkv = low_back(jnp.dot(branch_input_first, w_in[:, :3 * width], precision=HIGH, preferred_element_type=jnp.float32) + bias_qkv)
    hidden = low_back(jnp.dot(branch_input_second, w_in[:, 3 * width:], precision=HIGH, preferred_element_type=jnp.float32) + bias_hidden)
    cosine, sine = tables(doc)
    query = low(rotate(qkv[:, :width].reshape(slots, heads, HEAD), cosine, sine))
    keys = low(rotate(qkv[:, width:2 * width].reshape(slots, heads, HEAD), cosine, sine))
    values = low(qkv[:, 2 * width:].reshape(slots, heads, HEAD))
    raw = low_back(jnp.einsum('qhd,khd->hqk', query, keys, precision=HIGH) * HEAD ** (-0.5))
    rows = jnp.arange(slots)[:, None]
    cols = jnp.arange(slots)[None, :]
    allowed = (doc[:, None] == doc[None, :]) & (cols <= rows)
    scores = jnp.where(allowed[None], raw, NEG)
    probs = low(jax.nn.softmax(scores, axis=-1))
    attended = jnp.einsum('hqk,khd->qhd', probs, values, precision=HIGH).reshape(slots, width)
    attended = low(low_back(attended))
    active = low(jax.nn.gelu(hidden, approximate=False))
    joined = jnp.concatenate([attended, active], axis=1)
    return residual_stream + jnp.dot(joined, w_out, precision=HIGH, preferred_element_type=jnp.float32) + packed[11]

def adam(master, moment, square, grad, decay):
    moment_next = 0.9 * moment + 0.1 * grad
    square_next = 0.95 * square + 0.05 * grad * grad
    ratio = moment_next / (1.0 - 0.9 ** STEP) / (jnp.sqrt(square_next / (1.0 - 0.95 ** STEP)) + 1e-08)
    return (-0.03 * (ratio + decay * master), moment_next, square_next)

def reference(inputs, cotangent, doc_ids, master_in, master_out, vectors, moment_in, moment_out, moment_vec, square_in, square_out, square_vec):
    devices = inputs.shape[0] // SLOTS
    blocks_x = inputs.astype(jnp.float32).reshape(devices, SLOTS, D)
    blocks_c = cotangent.astype(jnp.float32).reshape(devices, SLOTS, D)
    blocks_d = doc_ids.reshape(devices, SLOTS)

    def one_device(carry, item):
        x_block, cot_block, doc_block = item
        live = (doc_block < SEQ_DEV).astype(jnp.float32)[:, None]

        def run(xv, wi, wo, vc):
            return forward(xv, wi, wo, vc, doc_block)
        result, pull = jax.vjp(run, x_block, master_in, master_out, vectors)
        gradient_stream, g_in, g_out, g_vec = pull(cot_block * live)
        carry = (carry[0] + g_in, carry[1] + g_out, carry[2] + g_vec)
        return (carry, ((result * live).astype(jnp.bfloat16), gradient_stream))
    start = (jnp.zeros(master_in.shape, jnp.float32), jnp.zeros(master_out.shape, jnp.float32), jnp.zeros(vectors.shape, jnp.float32))
    sums, stacked = lax.scan(one_device, start, (blocks_x, blocks_c, blocks_d))
    grad_in, grad_out, grad_vec = sums
    update_in, moment_in_next, square_in_next = adam(master_in, moment_in, square_in, grad_in, 0.1)
    update_out, moment_out_next, square_out_next = adam(master_out, moment_out, square_out, grad_out, 0.1)
    update_vec, moment_vec_next, square_vec_next = adam(vectors, moment_vec, square_vec, grad_vec, 0.0)
    output = stacked[0].reshape(devices * SLOTS, D)
    input_grad = stacked[1].reshape(devices * SLOTS, D)
    return (output, input_grad, grad_in, grad_out, grad_vec, update_in, update_out, update_vec, moment_in_next, moment_out_next, moment_vec_next, square_in_next, square_out_next, square_vec_next)
```

```python
import functools

import jax
import jax.numpy as jnp
from jax import lax
from jax.experimental import pallas as pl
from jax.experimental.pallas import tpu as pltpu
from jax.sharding import PartitionSpec as P

HEAD = 64
ROT = 16
SEQ_DEV = 1
STEP = 10


NEG = -1e30


def rotary_tables(doc_ids):
    count = doc_ids.shape[0]
    order = jnp.arange(count, dtype=jnp.int32)
    first = jnp.sum((doc_ids[None, :] < doc_ids[:, None]).astype(jnp.int32), axis=1)
    position = (order - first).astype(jnp.float32)
    half = ROT // 2
    freq = 10000.0 ** (-(jnp.arange(half, dtype=jnp.float32) * 2.0 / ROT))
    angle = position[:, None] * freq[None, :]
    angle = jnp.concatenate([angle, angle], axis=1)
    return (jnp.cos(angle), jnp.sin(angle))


def rotate(values, cosine, sine):
    half = ROT // 2
    part = values[..., :ROT]
    turned = jnp.concatenate([-part[..., half:], part[..., :half]], axis=-1)
    moved = part * cosine[:, None, :] + turned * sine[:, None, :]
    return jnp.concatenate([moved, values[..., ROT:]], axis=-1)


def rotate_back(grads, cosine, sine):
    half = ROT // 2
    part = grads[..., :ROT]
    scaled = part * sine[:, None, :]
    turned = jnp.concatenate([scaled[..., half:], -scaled[..., :half]], axis=-1)
    moved = part * cosine[:, None, :] + turned
    return jnp.concatenate([moved, grads[..., ROT:]], axis=-1)


def layer_norm_apply(residual_stream, norm_gain, norm_offset):
    feature_mean = jnp.mean(residual_stream, axis=-1, keepdims=True)
    mean_removed = residual_stream - feature_mean
    var = jnp.mean(mean_removed * mean_removed, axis=-1, keepdims=True)
    inverse_deviation = lax.rsqrt(var + 1e-05)
    normalized_input = mean_removed * inverse_deviation
    return (normalized_input * norm_gain + norm_offset, normalized_input, inverse_deviation)


def layer_norm_gradient(gradient_norm_output, normalized_input, inverse_deviation, norm_gain):
    gradient_normalized = gradient_norm_output * norm_gain
    gradient_stream = inverse_deviation * (
        gradient_normalized
        - jnp.mean(gradient_normalized, axis=-1, keepdims=True)
        - normalized_input
        * jnp.mean(gradient_normalized * normalized_input, axis=-1, keepdims=True)
    )
    return (
        gradient_stream,
        jnp.sum(gradient_norm_output * normalized_input, axis=0),
        jnp.sum(gradient_norm_output, axis=0),
    )


def unpack(packed, width):
    vec = packed.astype(jnp.float32)
    return (
        vec[0],
        vec[1],
        vec[2],
        vec[3],
        vec[4:7].reshape(3 * width),
        vec[7:11].reshape(4 * width),
        vec[11],
    )


def mask_block(doc_ids, start, stop):
    rows = jnp.arange(start, stop)[:, None]
    cols = jnp.arange(stop)[None, :]
    return (doc_ids[start:stop, None] == doc_ids[None, :stop]) & (cols <= rows)


def block_scores(query, keys, allowed, scale):
    raw = jnp.einsum("qhd,khd->hqk", query, keys, preferred_element_type=jnp.float32) * scale
    return jnp.where(allowed[None], raw, NEG)


def gelu_value(hidden):
    return 0.5 * hidden * (1.0 + lax.erf(hidden * 0.7071067811865476))


def gelu_slope(hidden):
    return (
        0.5 * (1.0 + lax.erf(hidden * 0.7071067811865476))
        + hidden * jnp.exp(-0.5 * hidden * hidden) * 0.3989422804014327
    )


def contract_rows(left, right):
    return lax.dot_general(
        left, right, (((0,), (0,)), ((), ())), preferred_element_type=jnp.float32
    )


def contract_cols(left, right):
    return lax.dot_general(
        left, right, (((1,), (1,)), ((), ())), preferred_element_type=jnp.float32
    )


def adam(master, moment, square, grad, decay):
    moment_next = 0.9 * moment + 0.1 * grad
    square_next = 0.95 * square + 0.05 * grad * grad
    ratio = moment_next / (1.0 - 0.9**STEP) / (jnp.sqrt(square_next / (1.0 - 0.95**STEP)) + 1e-08)
    return (-0.03 * (ratio + decay * master), moment_next, square_next)


def ring_position(shard, count):
    row, column = shard // 2, shard % 2
    return row + column * (count - 1 - 2 * row)


def ring_shard(position, count):
    upper = position // (count // 2)
    return 2 * position + upper * (2 * count - 1 - 4 * position)


class Stream:
    def __init__(self, rows, cols, axis):
        self.rows, self.cols, self.axis = rows, cols, axis
        self.unit = 16 if axis == 0 else 128
        self.half = (rows if axis == 0 else cols) // self.unit // 2
        self.outer = (2 * self.half + 3) // 6
        self.inner = self.half - 2 * self.outer

    def size(self, region):
        return self.inner if region == "b" else self.outer

    def shape(self, region):
        length = self.size(region) * self.unit
        return (length, self.cols) if self.axis == 0 else (self.rows, length)

    def piece(self, ref, row, core, side, region):
        if region == "b":
            offset = self.outer
        elif region == "a":
            offset = side * (self.half - self.outer)
        else:
            offset = (1 - side) * (self.half - self.outer)
        begin = pl.multiple_of((core * self.half + offset) * self.unit, self.unit)
        if self.axis == 0:
            begin = pl.multiple_of(row + begin, 16)
            return ref.at[pl.ds(begin, self.shape(region)[0]), :]
        row = row if isinstance(row, int) else pl.multiple_of(row, 16)
        return ref.at[pl.ds(row, self.rows), pl.ds(begin, self.shape(region)[1])]


def streams_of(in_rows, out_rows, width):
    return (
        Stream(in_rows, 3 * width, 1),
        Stream(in_rows, 4 * width, 1),
        Stream(out_rows, width, 0),
    )


def remote(source, target, send, receive, device):
    return pltpu.make_async_remote_copy(
        src_ref=source,
        dst_ref=target,
        send_sem=send,
        recv_sem=receive,
        device_id=device,
        device_id_type=pl.DeviceIdType.MESH,
    )


def places(count):
    group = lax.axis_index("grp")
    me = lax.axis_index("shard")
    core, side = group % 2, group // 2
    position = ring_position(me, count)
    after = ring_shard((position + 1) % count, count)
    before = ring_shard((position + count - 1) % count, count)
    across = {"grp": (1 - side) * 2 + core}
    partner = {"grp": side * 2 + 1 - core}
    return group, me, core, side, position, {"shard": after}, {"shard": before}, across, partner


def greet(me, count, devices):
    barrier = pltpu.get_barrier_semaphore()

    def hello(step, carry):
        pl.semaphore_signal(
            barrier,
            inc=1,
            device_id={"shard": (me + step) % count},
            device_id_type=pl.DeviceIdType.MESH,
        )
        return carry

    lax.fori_loop(1, count, hello, 0)
    for device in devices:
        pl.semaphore_signal(
            barrier, inc=1, device_id=device, device_id_type=pl.DeviceIdType.MESH
        )
    pl.semaphore_wait(barrier, count - 1 + len(devices))


def gather_kernel(count, streams, in_ref, out_ref, vec_ref, q_ref, h_ref, o_ref, v_ref, *sems):
    (ring_a_s, ring_a_r, ring_b_s, ring_b_r, side_s, side_r) = sems[:6]
    (core_a_s, core_a_r, core_b_s, core_b_r, core_x_s, core_x_r) = sems[6:12]
    vec_s, vec_r, own = sems[12:]
    _, me, core, side, position, after, before, across, partner = places(count)
    full = (q_ref, h_ref, o_ref)
    kinds = range(len(streams))
    split = streams[0].cols
    shard_refs = (in_ref.at[:, pl.ds(0, split)], in_ref.at[:, pl.ds(split, streams[1].cols)], out_ref)
    own_copies = [
        pltpu.make_async_copy(
            shard_refs[k],
            full[k].at[pl.ds(pl.multiple_of(me * streams[k].rows, 16), streams[k].rows), :],
            own.at[k],
        )
        for k in kinds
    ]
    own_copies.append(pltpu.make_async_copy(vec_ref, v_ref.at[me], own.at[len(streams)]))
    for copy in own_copies:
        copy.start()
    greet(me, count, (across, partner))

    def piece(k, shard, region):
        return streams[k].piece(full[k], shard * streams[k].rows, core, side, region)

    def first(k, region):
        return streams[k].piece(shard_refs[k], 0, core, side, region)

    def ring_a(k, step, shard, source=None):
        target = piece(k, shard, "a")
        source = target if source is None else source
        return remote(source, target, ring_a_s.at[k, step], ring_a_r.at[k, step], after)

    def ring_b(k, step, shard, source=None):
        target = piece(k, shard, "b")
        source = target if source is None else source
        return remote(source, target, ring_b_s.at[k, step], ring_b_r.at[k, step], before)

    def side_a(k, step, shard):
        target = piece(k, shard, "a")
        return remote(target, target, side_s.at[k, step], side_r.at[k, step], across)

    def core_copy(k, step, shard, region):
        send, receive = {
            "a": (core_a_s, core_a_r),
            "b": (core_b_s, core_b_r),
            "x": (core_x_s, core_x_r),
        }[region]
        target = piece(k, shard, region)
        return remote(target, target, send.at[k, step], receive.at[k, step], partner)

    def shard_a(step):
        return ring_shard((position + 2 * count - 1 - step) % count, count)

    def shard_b(step):
        return ring_shard((position + 1 + step) % count, count)

    for k in kinds:
        ring_a(k, 0, me, first(k, "a")).start()
        ring_b(k, 0, me, first(k, "b")).start()

    def vec_copy(step):
        return remote(
            vec_ref,
            v_ref.at[me],
            vec_s.at[step],
            vec_r.at[step],
            {"shard": (me + step) % count},
        )

    def send_vec(step, carry):
        vec_copy(step).start()
        return carry

    lax.fori_loop(1, count, send_vec, 0)

    def handle_side(step):
        shard = shard_a(step)
        for k in kinds:
            taken = piece(k, shard, "x")
            remote(taken, taken, side_s.at[k, step], side_r.at[k, step], across).wait_recv()
            core_copy(k, step, shard, "x").start()

    def body(step, is_first, is_last):
        come_a, come_b = shard_a(step), shard_b(step)
        for k in kinds:
            ring_a(k, step, come_a).wait_recv()
            if not is_last:
                ring_a(k, step + 1, come_a).start()
            side_a(k, step, come_a).start()
            core_copy(k, step, come_a, "a").start()
            ring_b(k, step, come_b).wait_recv()
            if not is_last:
                ring_b(k, step + 1, come_b).start()
            core_copy(k, step, come_b, "b").start()
        if not is_first:
            handle_side(step - 1)

    def middle(step, carry):
        body(step, False, False)
        return carry

    body(0, True, False)
    lax.fori_loop(1, count - 2, middle, 0)
    body(count - 2, False, True)
    handle_side(count - 2)

    def finish(step, carry):
        come_a, come_b = shard_a(step), shard_b(step)
        for k in kinds:
            ring_a(k, step, come_a).wait_send()
            ring_b(k, step, come_b).wait_send()
            side_a(k, step, come_a).wait_send()
            for region, shard in (("a", come_a), ("b", come_b), ("x", come_a)):
                copy = core_copy(k, step, shard, region)
                copy.wait_send()
                copy.wait_recv()
        return carry

    lax.fori_loop(0, count - 1, finish, 0)

    def finish_vec(step, carry):
        vec_copy(step).wait_send()
        vec_copy(step).wait_recv()
        return carry

    lax.fori_loop(1, count, finish_vec, 0)
    for copy in own_copies:
        copy.wait()


def gather_weights(w_in, w_out, packed, count):
    in_rows, out_rows, width = w_in.shape[0], w_out.shape[0], w_out.shape[1]
    streams = streams_of(in_rows, out_rows, width)
    kinds, steps = len(streams), count - 1
    dma = pltpu.SemaphoreType.DMA
    return pl.pallas_call(
        functools.partial(gather_kernel, count, streams),
        out_shape=[
            jax.ShapeDtypeStruct((count * in_rows, 3 * width), jnp.bfloat16),
            jax.ShapeDtypeStruct((count * in_rows, 4 * width), jnp.bfloat16),
            jax.ShapeDtypeStruct((count * out_rows, width), jnp.bfloat16),
            jax.ShapeDtypeStruct((count,) + packed.shape, jnp.bfloat16),
        ],
        in_specs=[pl.BlockSpec(memory_space=pltpu.VMEM)] * 3,
        out_specs=[pl.BlockSpec(memory_space=pl.ANY)] * 4,
        scratch_shapes=[dma((kinds, steps))] * 12 + [dma((count,)), dma((count,)), dma((kinds + 1,))],
        compiler_params=pltpu.CompilerParams(collective_id=0, has_side_effects=True),
        name="gather_weights",
    )(w_in, w_out, packed)


def add_into(target, sources):
    rows = target.shape[0]
    block = 16

    def add(index, carry):
        at = pl.ds(pl.multiple_of(index * block, block), block)
        total = target[at, :].astype(jnp.float32)
        for source in sources:
            total = total + source[at, :].astype(jnp.float32)
        target[at, :] = total.astype(jnp.bfloat16)
        return carry

    lax.fori_loop(0, rows // block, add, 0)


def reduce_kernel(count, streams, *refs):
    kinds = range(len(streams))
    kind_count = len(streams)
    given, vec_ref = refs[:3], refs[3]
    final, vec_out = refs[4:7], refs[7]
    refs = refs[8:]
    mine = {r: refs[kind_count * n : kind_count * (n + 1)] for n, r in enumerate("abx")}
    refs = refs[3 * kind_count :]
    other = {r: refs[kind_count * n : kind_count * (n + 1)] for n, r in enumerate("abx")}
    refs = refs[3 * kind_count :]
    from_side, from_a, from_b, last_b, end_b = (
        refs[kind_count * n : kind_count * (n + 1)] for n in range(5)
    )
    refs = refs[5 * kind_count :]
    vec_mine, vec_come, vec_all = refs[:3]
    load, core_s, core_r = refs[3:6]
    side_s, side_r, ring_a_s, ring_a_r, ring_b_s, ring_b_r = refs[6:12]
    end_s, end_r, put = refs[12:15]
    vec_s, vec_r, vec_gs, vec_gr, vec_own = refs[15:]
    group, me, core, side, position, after, before, across, partner = places(count)

    def target_of(step, region):
        if region == "b":
            return ring_shard((position + 1 + step) % count, count)
        return ring_shard((position + 2 * count - 1 - step) % count, count)

    def given_piece(k, step, region, half):
        row = target_of(step, region) * streams[k].rows
        return streams[k].piece(given[k], row, half, side, region)

    def load_copy(k, step, region):
        number = "abx".index(region)
        return pltpu.make_async_copy(
            given_piece(k, step, region, core), mine[region][k].at[step], load.at[number, k, step]
        )

    def core_copy(k, step, region):
        number = "abx".index(region)
        return remote(
            given_piece(k, step, region, 1 - core),
            other[region][k].at[step],
            core_s.at[number, k, step],
            core_r.at[number, k, step],
            partner,
        )

    def begin_load(step, carry):
        for region in "xba":
            for k in kinds:
                load_copy(k, step, region).start()
        return carry

    def begin_core(step, carry):
        for region in "xba":
            for k in kinds:
                core_copy(k, step, region).start()
        return carry

    vec_load = pltpu.make_async_copy(vec_ref.at[me], vec_mine, vec_own.at[0])
    vec_load.start()
    lax.fori_loop(0, count, begin_load, 0)
    greet(me, count, (across, partner, {"grp": (1 - side) * 2 + 1 - core}))
    lax.fori_loop(0, count, begin_core, 0)

    def vec_copy(step):
        to = (me + step) % count
        return remote(
            vec_ref.at[to], vec_come.at[step], vec_s.at[step], vec_r.at[step], {"shard": to}
        )

    def send_vec(step, carry):
        vec_copy(step).start()
        return carry

    lax.fori_loop(1, count, send_vec, 0)

    def side_copy(k, step):
        return remote(
            mine["x"][k].at[step],
            from_side[k].at[step],
            side_s.at[k, step],
            side_r.at[k, step],
            across,
        )

    def ring_a(k, step):
        return remote(
            mine["a"][k].at[step],
            from_a[k].at[step],
            ring_a_s.at[k, step],
            ring_a_r.at[k, step],
            after,
        )

    def ring_b(k, step):
        return remote(
            mine["b"][k].at[step],
            from_b[k].at[step],
            ring_b_s.at[k, step],
            ring_b_r.at[k, step],
            before,
        )

    def ready(k, step, region):
        load_copy(k, step, region).wait()
        core_copy(k, step, region).wait_recv()

    def give_side(step):
        for k in kinds:
            ready(k, step, "x")
            add_into(mine["x"][k].at[step], [other["x"][k].at[step]])
            side_copy(k, step).start()

    def body(step, is_first, is_last):
        for k in kinds:
            ready(k, step, "b")
            terms = [other["b"][k].at[step]]
            if not is_first:
                ring_b(k, step - 1).wait_recv()
                terms.append(from_b[k].at[step - 1])
            add_into(mine["b"][k].at[step], terms)
            if not is_last:
                ring_b(k, step).start()
            ready(k, step, "a")
            side_copy(k, step).wait_recv()
            terms = [other["a"][k].at[step], from_side[k].at[step]]
            if not is_first:
                ring_a(k, step - 1).wait_recv()
                terms.append(from_a[k].at[step - 1])
            add_into(mine["a"][k].at[step], terms)
            if not is_last:
                ring_a(k, step).start()
        if not is_last:
            give_side_next(step)

    def give_side_next(step):
        @pl.when(step + 2 < count)
        def _():
            give_side(step + 2)

    def middle(step, carry):
        body(step, False, False)
        return carry

    give_side(0)
    give_side(1)
    body(0, True, False)
    lax.fori_loop(1, count - 1, middle, 0)
    body(count - 1, False, True)

    last = count - 1

    def final_piece(k, region):
        return streams[k].piece(final[k], 0, core, side, region)

    def end_swap(k):
        return remote(mine["b"][k].at[last], last_b[k], end_s.at[0, k], end_r.at[0, k], across)

    def end_side(k):
        place = final_piece(k, "a")
        return remote(mine["a"][k].at[last], place, end_s.at[1, k], end_r.at[1, k], across)

    def end_core(k, number, region, source):
        place = final_piece(k, region)
        return remote(source, place, end_s.at[number, k], end_r.at[number, k], partner)

    for k in kinds:
        end_swap(k).start()
        end_side(k).start()
    puts = []
    cores = []
    for k in kinds:
        puts.append(
            pltpu.make_async_copy(mine["a"][k].at[last], final_piece(k, "a"), put.at[0, k])
        )
        cores.append(end_core(k, 2, "a", mine["a"][k].at[last]))
        puts[-1].start()
        cores[-1].start()

    def vec_wait(step, carry):
        vec_copy(step).wait_recv()
        return carry

    lax.fori_loop(1, count, vec_wait, 0)
    vec_load.wait()
    vec_come[0] = vec_mine[...]
    total = vec_come[me % count]
    for shard in range(1, count):
        total = total + vec_come[(me + count - shard) % count]
    vec_mine[...] = total
    vec_keep = pltpu.make_async_copy(vec_mine, vec_all.at[group], vec_own.at[1])
    vec_keep.start()

    def vec_group(step):
        return remote(
            vec_mine,
            vec_all.at[group],
            vec_gs.at[step],
            vec_gr.at[step],
            {"grp": (group + step) % 4},
        )

    for step in range(1, 4):
        vec_group(step).start()

    for k in kinds:
        end_swap(k).wait_recv()
        rows = last_b[k].shape[0]

        def add(index, carry, k=k):
            at = pl.ds(pl.multiple_of(index * 16, 16), 16)
            both = mine["b"][k][last, at, :].astype(jnp.float32) + last_b[k][at, :].astype(
                jnp.float32
            )
            end_b[k][at, :] = both.astype(jnp.bfloat16)
            return carry

        lax.fori_loop(0, rows // 16, add, 0)
        puts.append(pltpu.make_async_copy(end_b[k], final_piece(k, "b"), put.at[1, k]))
        cores.append(end_core(k, 3, "b", end_b[k]))
        puts[-1].start()
        cores[-1].start()
        place = final_piece(k, "x")
        remote(place, place, end_s.at[1, k], end_r.at[1, k], across).wait_recv()
        cores.append(end_core(k, 4, "x", place))
        cores[-1].start()

    vec_keep.wait()
    for step in range(1, 4):
        vec_group(step).wait_recv()
    vec_out[...] = vec_all[0] + vec_all[1] + vec_all[2] + vec_all[3]
    for step in range(1, 4):
        vec_group(step).wait_send()

    def finish_vec(step, carry):
        vec_copy(step).wait_send()
        return carry

    lax.fori_loop(1, count, finish_vec, 0)

    def finish_core(step, carry):
        for k in kinds:
            for region in "xba":
                core_copy(k, step, region).wait_send()
            side_copy(k, step).wait_send()
        return carry

    lax.fori_loop(0, count, finish_core, 0)

    def finish_ring(step, carry):
        for k in kinds:
            ring_a(k, step).wait_send()
            ring_b(k, step).wait_send()
        return carry

    lax.fori_loop(0, count - 1, finish_ring, 0)
    for k in kinds:
        end_swap(k).wait_send()
        end_side(k).wait_send()
    for copy in puts:
        copy.wait()
    for copy in cores:
        copy.wait_send()
        copy.wait_recv()


def reduce_grads(grad_qkv, grad_hidden, grad_out, grad_vec, count):
    width = grad_out.shape[1]
    in_rows, out_rows = grad_qkv.shape[0] // count, grad_out.shape[0] // count
    streams = streams_of(in_rows, out_rows, width)
    kinds = len(streams)
    dma = pltpu.SemaphoreType.DMA

    def slots(number, region):
        return [pltpu.VMEM((number,) + s.shape(region), jnp.bfloat16) for s in streams]

    slab = grad_vec.shape[1:]
    return pl.pallas_call(
        functools.partial(reduce_kernel, count, streams),
        out_shape=[
            jax.ShapeDtypeStruct((in_rows, 3 * width), jnp.bfloat16),
            jax.ShapeDtypeStruct((in_rows, 4 * width), jnp.bfloat16),
            jax.ShapeDtypeStruct((out_rows, width), jnp.bfloat16),
            jax.ShapeDtypeStruct(slab, jnp.float32),
        ],
        in_specs=[pl.BlockSpec(memory_space=pl.ANY)] * 4,
        out_specs=[pl.BlockSpec(memory_space=pl.ANY)] * 3
        + [pl.BlockSpec(memory_space=pltpu.VMEM)],
        scratch_shapes=slots(count, "a")
        + slots(count, "b")
        + slots(count, "x")
        + slots(count, "a")
        + slots(count, "b")
        + slots(count, "x")
        + slots(count, "a")
        + slots(count - 1, "a")
        + slots(count - 1, "b")
        + [pltpu.VMEM(s.shape("b"), jnp.bfloat16) for s in streams] * 2
        + [
            pltpu.VMEM(slab, jnp.float32),
            pltpu.VMEM((count,) + slab, jnp.float32),
            pltpu.VMEM((4,) + slab, jnp.float32),
            dma((3, kinds, count)),
            dma((3, kinds, count)),
            dma((3, kinds, count)),
            dma((kinds, count)),
            dma((kinds, count)),
            dma((kinds, count)),
            dma((kinds, count)),
            dma((kinds, count)),
            dma((kinds, count)),
            dma((5, kinds)),
            dma((5, kinds)),
            dma((2, kinds)),
            dma((count,)),
            dma((count,)),
            dma((4,)),
            dma((4,)),
            dma((2,)),
        ],
        compiler_params=pltpu.CompilerParams(
            collective_id=1, has_side_effects=True, vmem_limit_bytes=60000000
        ),
        name="reduce_grads",
    )(grad_qkv, grad_hidden, grad_out, grad_vec)


def shards(
    count,
    inputs,
    cotangent,
    doc_ids,
    master_in,
    master_out,
    vectors,
    moment_in,
    moment_out,
    moment_vec,
    square_in,
    square_out,
    square_vec,
):
    slots, width = inputs.shape
    heads = width // HEAD
    block = min(512, slots)
    scale = HEAD ** (-0.5)
    live = (doc_ids < SEQ_DEV).astype(jnp.float32)[:, None]
    cosine, sine = rotary_tables(doc_ids)
    w_qkv, w_hidden, w_out, packed = gather_weights(
        master_in.astype(jnp.bfloat16),
        master_out.astype(jnp.bfloat16),
        jnp.pad(vectors, ((0, 4), (0, 0))).astype(jnp.bfloat16),
        count,
    )
    packed = packed.transpose(1, 0, 2).reshape(16, width)
    (
        first_norm_gain,
        first_norm_offset,
        second_norm_gain,
        second_norm_offset,
        bias_qkv,
        bias_hidden,
        bias_out,
    ) = unpack(packed, width)
    residual_stream = inputs.astype(jnp.float32)
    branch_input_first, first_normalized, first_inverse_deviation = layer_norm_apply(
        residual_stream, first_norm_gain, first_norm_offset
    )
    branch_input_second, second_normalized, second_inverse_deviation = layer_norm_apply(
        residual_stream, second_norm_gain, second_norm_offset
    )
    branch_input_first = branch_input_first.astype(jnp.bfloat16)
    branch_input_second = branch_input_second.astype(jnp.bfloat16)
    qkv = (
        jnp.dot(branch_input_first, w_qkv, preferred_element_type=jnp.float32)
        + bias_qkv
    )
    hidden = (
        jnp.dot(branch_input_second, w_hidden, preferred_element_type=jnp.float32)
        + bias_hidden
    )
    query = rotate(qkv[:, :width].reshape(slots, heads, HEAD), cosine, sine).astype(jnp.bfloat16)
    keys = rotate(qkv[:, width : 2 * width].reshape(slots, heads, HEAD), cosine, sine).astype(
        jnp.bfloat16
    )
    values = qkv[:, 2 * width :].reshape(slots, heads, HEAD).astype(jnp.bfloat16)
    start = 0
    stop = start + block
    allowed = mask_block(doc_ids, start, stop)
    scores = block_scores(query, keys, allowed, scale)
    top = jnp.max(scores, axis=-1, keepdims=True)
    expo = jnp.exp(scores - top)
    total = jnp.sum(expo, axis=-1, keepdims=True)
    probs = (expo / total).astype(jnp.bfloat16)
    totals = [top + jnp.log(total)]
    attended_parts = jnp.einsum("hqk,khd->qhd", probs, values, preferred_element_type=jnp.float32)
    attended = attended_parts.reshape(slots, width).astype(jnp.bfloat16)
    active = gelu_value(hidden).astype(jnp.bfloat16)
    joined = jnp.concatenate([attended, active], axis=1)
    branch = jnp.dot(joined, w_out, preferred_element_type=jnp.float32) + bias_out
    output = ((residual_stream + branch) * live).astype(jnp.bfloat16)
    d_out = cotangent.astype(jnp.float32) * live
    d_out_low = d_out.astype(jnp.bfloat16)
    d_joined = contract_cols(d_out_low, w_out)
    grad_out_term = contract_rows(joined, d_out_low)
    d_attended = d_joined[:, :width].reshape(slots, heads, HEAD).astype(jnp.bfloat16)
    d_hidden = (d_joined[:, width:] * gelu_slope(hidden)).astype(jnp.bfloat16)
    d_query_parts = []
    d_keys = jnp.zeros((slots, heads, HEAD), jnp.float32)
    d_values = jnp.zeros((slots, heads, HEAD), jnp.float32)
    for number, start in enumerate(range(0, slots, block)):
        stop = start + block
        allowed = mask_block(doc_ids, start, stop)
        scores = block_scores(query, keys, allowed, scale)
        probs = jnp.exp(scores - totals[number])
        d_probs = jnp.einsum("qhd,khd->hqk", d_attended, values, preferred_element_type=jnp.float32)
        weighted = jnp.sum(probs * d_probs, axis=-1, keepdims=True)
        d_scores = (probs * (d_probs - weighted)).astype(jnp.bfloat16)
        d_query_parts.append(
            jnp.einsum("hqk,khd->qhd", d_scores, keys, preferred_element_type=jnp.float32) * scale
        )
        d_keys = d_keys.at[:stop].add(
            jnp.einsum("hqk,qhd->khd", d_scores, query, preferred_element_type=jnp.float32) * scale
        )
        d_values = d_values.at[:stop].add(
            jnp.einsum(
                "hqk,qhd->khd",
                probs.astype(jnp.bfloat16),
                d_attended,
                preferred_element_type=jnp.float32,
            )
        )
    d_query = rotate_back(d_query_parts[0], cosine, sine)
    d_keys = rotate_back(d_keys, cosine, sine)
    d_qkv = jnp.concatenate(
        [
            d_query.reshape(slots, width),
            d_keys.reshape(slots, width),
            d_values.reshape(slots, width),
        ],
        axis=1,
    ).astype(jnp.bfloat16)
    grad_qkv_term = contract_rows(branch_input_first, d_qkv)
    grad_hidden_term = contract_rows(branch_input_second, d_hidden)
    gradient_branch_first = contract_cols(d_qkv, w_qkv)
    gradient_branch_second = contract_cols(d_hidden, w_hidden)
    gradient_stream_first, gradient_gain_first, gradient_offset_first = layer_norm_gradient(
        gradient_branch_first, first_normalized, first_inverse_deviation, first_norm_gain
    )
    gradient_stream_second, gradient_gain_second, gradient_offset_second = layer_norm_gradient(
        gradient_branch_second, second_normalized, second_inverse_deviation, second_norm_gain
    )
    input_grad = d_out + gradient_stream_first + gradient_stream_second
    grad_vec_term = jnp.concatenate(
        [
            gradient_gain_first[None],
            gradient_offset_first[None],
            gradient_gain_second[None],
            gradient_offset_second[None],
            jnp.sum(d_qkv, axis=0, dtype=jnp.float32).reshape(3, width),
            jnp.sum(d_hidden, axis=0, dtype=jnp.float32).reshape(4, width),
            jnp.sum(d_out, axis=0)[None],
        ],
        axis=0,
    )
    vec_slabs = jnp.pad(grad_vec_term, ((0, 4), (0, 0)))
    vec_slabs = vec_slabs.reshape(16, count, width // count).transpose(1, 0, 2)
    sum_qkv, sum_hidden, sum_out, sum_vec = reduce_grads(
        grad_qkv_term.astype(jnp.bfloat16),
        grad_hidden_term.astype(jnp.bfloat16),
        grad_out_term.astype(jnp.bfloat16),
        vec_slabs,
        count,
    )
    grad_in = jnp.concatenate([sum_qkv, sum_hidden], axis=1).astype(jnp.float32)
    grad_out = sum_out.astype(jnp.float32)
    grad_vec = sum_vec[:12]
    update_in, moment_in_next, square_in_next = adam(master_in, moment_in, square_in, grad_in, 0.1)
    update_out, moment_out_next, square_out_next = adam(
        master_out, moment_out, square_out, grad_out, 0.1
    )
    update_vec, moment_vec_next, square_vec_next = adam(
        vectors, moment_vec, square_vec, grad_vec, 0.0
    )
    return (
        output,
        input_grad,
        grad_in,
        grad_out,
        grad_vec,
        update_in,
        update_out,
        update_vec,
        moment_in_next,
        moment_out_next,
        moment_vec_next,
        square_in_next,
        square_out_next,
        square_vec_next,
    )


def solution(mesh):
    placed = (
        P(("grp", "shard"), None),
        P(("grp", "shard"), None),
        P(("grp", "shard")),
        P("shard", None),
        P("shard", None),
        P(None, "shard"),
        P("shard", None),
        P("shard", None),
        P(None, "shard"),
        P("shard", None),
        P("shard", None),
        P(None, "shard"),
    )
    return jax.shard_map(
        functools.partial(shards, mesh.shape["shard"]),
        mesh=mesh,
        in_specs=placed,
        out_specs=(
            P(("grp", "shard"), None),
            P(("grp", "shard"), None),
            P("shard", None),
            P("shard", None),
            P(None, "shard"),
            P("shard", None),
            P("shard", None),
            P(None, "shard"),
            P("shard", None),
            P("shard", None),
            P(None, "shard"),
            P("shard", None),
            P("shard", None),
            P(None, "shard"),
        ),
        check_vma=False,
    )
```

```python
import functools

import jax
import jax.numpy as jnp
from jax import lax
from jax.experimental import pallas as pl
from jax.experimental.pallas import tpu as pltpu
from jax.sharding import PartitionSpec as P

HEAD = 64
ROT = 16
SEQ_DEV = 1
STEP = 10


NEG = -1e30


def rotary_tables(doc_ids):
    count = doc_ids.shape[0]
    order = jnp.arange(count, dtype=jnp.int32)
    first = jnp.sum((doc_ids[None, :] < doc_ids[:, None]).astype(jnp.int32), axis=1)
    position = (order - first).astype(jnp.float32)
    half = ROT // 2
    freq = 10000.0 ** (-(jnp.arange(half, dtype=jnp.float32) * 2.0 / ROT))
    angle = position[:, None] * freq[None, :]
    angle = jnp.concatenate([angle, angle], axis=1)
    return (jnp.cos(angle), jnp.sin(angle))


def rotate(values, cosine, sine):
    half = ROT // 2
    part = values[..., :ROT]
    turned = jnp.concatenate([-part[..., half:], part[..., :half]], axis=-1)
    moved = part * cosine[:, None, :] + turned * sine[:, None, :]
    return jnp.concatenate([moved, values[..., ROT:]], axis=-1)


def rotate_back(grads, cosine, sine):
    half = ROT // 2
    part = grads[..., :ROT]
    scaled = part * sine[:, None, :]
    turned = jnp.concatenate([scaled[..., half:], -scaled[..., :half]], axis=-1)
    moved = part * cosine[:, None, :] + turned
    return jnp.concatenate([moved, grads[..., ROT:]], axis=-1)


def layer_norm_apply(residual_stream, norm_gain, norm_offset):
    feature_mean = jnp.mean(residual_stream, axis=-1, keepdims=True)
    mean_removed = residual_stream - feature_mean
    var = jnp.mean(mean_removed * mean_removed, axis=-1, keepdims=True)
    inverse_deviation = lax.rsqrt(var + 1e-05)
    normalized_input = mean_removed * inverse_deviation
    return (normalized_input * norm_gain + norm_offset, normalized_input, inverse_deviation)


def layer_norm_gradient(gradient_norm_output, normalized_input, inverse_deviation, norm_gain):
    gradient_normalized = gradient_norm_output * norm_gain
    gradient_stream = inverse_deviation * (
        gradient_normalized
        - jnp.mean(gradient_normalized, axis=-1, keepdims=True)
        - normalized_input
        * jnp.mean(gradient_normalized * normalized_input, axis=-1, keepdims=True)
    )
    return (
        gradient_stream,
        jnp.sum(gradient_norm_output * normalized_input, axis=0),
        jnp.sum(gradient_norm_output, axis=0),
    )


def unpack(packed, width):
    vec = packed.astype(jnp.float32)
    return (
        vec[0],
        vec[1],
        vec[2],
        vec[3],
        vec[4:7].reshape(3 * width),
        vec[7:11].reshape(4 * width),
        vec[11],
    )


def mask_block(doc_ids, start, stop):
    rows = jnp.arange(start, stop)[:, None]
    cols = jnp.arange(stop)[None, :]
    return (doc_ids[start:stop, None] == doc_ids[None, :stop]) & (cols <= rows)


def block_scores(query, keys, allowed, scale):
    raw = jnp.einsum("qhd,khd->hqk", query, keys, preferred_element_type=jnp.float32) * scale
    return jnp.where(allowed[None], raw, NEG)


def gelu_value(hidden):
    return 0.5 * hidden * (1.0 + lax.erf(hidden * 0.7071067811865476))


def gelu_slope(hidden):
    return (
        0.5 * (1.0 + lax.erf(hidden * 0.7071067811865476))
        + hidden * jnp.exp(-0.5 * hidden * hidden) * 0.3989422804014327
    )


def contract_rows(left, right):
    return lax.dot_general(
        left, right, (((0,), (0,)), ((), ())), preferred_element_type=jnp.float32
    )


def contract_cols(left, right):
    return lax.dot_general(
        left, right, (((1,), (1,)), ((), ())), preferred_element_type=jnp.float32
    )


def adam(master, moment, square, grad, decay):
    moment_next = 0.9 * moment + 0.1 * grad
    square_next = 0.95 * square + 0.05 * grad * grad
    ratio = moment_next / (1.0 - 0.9**STEP) / (jnp.sqrt(square_next / (1.0 - 0.95**STEP)) + 1e-08)
    return (-0.03 * (ratio + decay * master), moment_next, square_next)


def ring_position(shard, count):
    row, column = shard // 2, shard % 2
    return row + column * (count - 1 - 2 * row)


def ring_shard(position, count):
    upper = position // (count // 2)
    return 2 * position + upper * (2 * count - 1 - 4 * position)


class Stream:
    def __init__(self, rows, cols, axis):
        self.rows, self.cols, self.axis = rows, cols, axis
        self.unit = 16 if axis == 0 else 128
        self.half = (rows if axis == 0 else cols) // self.unit // 2
        self.outer = (2 * self.half + 3) // 6
        self.inner = self.half - 2 * self.outer

    def size(self, region):
        return self.inner if region == "b" else self.outer

    def shape(self, region):
        length = self.size(region) * self.unit
        return (length, self.cols) if self.axis == 0 else (self.rows, length)

    def piece(self, ref, row, core, side, region):
        if region == "b":
            offset = self.outer
        elif region == "a":
            offset = side * (self.half - self.outer)
        else:
            offset = (1 - side) * (self.half - self.outer)
        begin = pl.multiple_of((core * self.half + offset) * self.unit, self.unit)
        if self.axis == 0:
            begin = pl.multiple_of(row + begin, 16)
            return ref.at[pl.ds(begin, self.shape(region)[0]), :]
        row = row if isinstance(row, int) else pl.multiple_of(row, 16)
        return ref.at[pl.ds(row, self.rows), pl.ds(begin, self.shape(region)[1])]


def streams_of(in_rows, out_rows, width):
    return (
        Stream(in_rows, 3 * width, 1),
        Stream(in_rows, 4 * width, 1),
        Stream(out_rows, width, 0),
    )


def remote(source, target, send, receive, device):
    return pltpu.make_async_remote_copy(
        src_ref=source,
        dst_ref=target,
        send_sem=send,
        recv_sem=receive,
        device_id=device,
        device_id_type=pl.DeviceIdType.MESH,
    )


def places(count):
    group = lax.axis_index("grp")
    me = lax.axis_index("shard")
    core, side = group % 2, group // 2
    position = ring_position(me, count)
    after = ring_shard((position + 1) % count, count)
    before = ring_shard((position + count - 1) % count, count)
    across = {"grp": (1 - side) * 2 + core}
    partner = {"grp": side * 2 + 1 - core}
    return group, me, core, side, position, {"shard": after}, {"shard": before}, across, partner


def greet(me, count, devices):
    barrier = pltpu.get_barrier_semaphore()

    def hello(step, carry):
        pl.semaphore_signal(
            barrier,
            inc=1,
            device_id={"shard": (me + step) % count},
            device_id_type=pl.DeviceIdType.MESH,
        )
        return carry

    lax.fori_loop(1, count, hello, 0)
    for device in devices:
        pl.semaphore_signal(
            barrier, inc=1, device_id=device, device_id_type=pl.DeviceIdType.MESH
        )
    pl.semaphore_wait(barrier, count - 1 + len(devices))


def gather_kernel(count, streams, in_ref, out_ref, vec_ref, q_ref, h_ref, o_ref, v_ref, *sems):
    (ring_a_s, ring_a_r, ring_b_s, ring_b_r, side_s, side_r) = sems[:6]
    (core_a_s, core_a_r, core_b_s, core_b_r, core_x_s, core_x_r) = sems[6:12]
    vec_s, vec_r, own = sems[12:]
    _, me, core, side, position, after, before, across, partner = places(count)
    full = (q_ref, h_ref, o_ref)
    kinds = range(len(streams))
    split = streams[0].cols
    shard_refs = (in_ref.at[:, pl.ds(0, split)], in_ref.at[:, pl.ds(split, streams[1].cols)], out_ref)
    own_copies = [
        pltpu.make_async_copy(
            shard_refs[k],
            full[k].at[pl.ds(pl.multiple_of(me * streams[k].rows, 16), streams[k].rows), :],
            own.at[k],
        )
        for k in kinds
    ]
    own_copies.append(pltpu.make_async_copy(vec_ref, v_ref.at[me], own.at[len(streams)]))
    for copy in own_copies:
        copy.start()
    greet(me, count, (across, partner))

    def piece(k, shard, region):
        return streams[k].piece(full[k], shard * streams[k].rows, core, side, region)

    def first(k, region):
        return streams[k].piece(shard_refs[k], 0, core, side, region)

    def ring_a(k, step, shard, source=None):
        target = piece(k, shard, "a")
        source = target if source is None else source
        return remote(source, target, ring_a_s.at[k, step], ring_a_r.at[k, step], after)

    def ring_b(k, step, shard, source=None):
        target = piece(k, shard, "b")
        source = target if source is None else source
        return remote(source, target, ring_b_s.at[k, step], ring_b_r.at[k, step], before)

    def side_a(k, step, shard):
        target = piece(k, shard, "a")
        return remote(target, target, side_s.at[k, step], side_r.at[k, step], across)

    def core_copy(k, step, shard, region):
        send, receive = {
            "a": (core_a_s, core_a_r),
            "b": (core_b_s, core_b_r),
            "x": (core_x_s, core_x_r),
        }[region]
        target = piece(k, shard, region)
        return remote(target, target, send.at[k, step], receive.at[k, step], partner)

    def shard_a(step):
        return ring_shard((position + 2 * count - 1 - step) % count, count)

    def shard_b(step):
        return ring_shard((position + 1 + step) % count, count)

    for k in kinds:
        ring_a(k, 0, me, first(k, "a")).start()
        ring_b(k, 0, me, first(k, "b")).start()

    def vec_copy(step):
        return remote(
            vec_ref,
            v_ref.at[me],
            vec_s.at[step],
            vec_r.at[step],
            {"shard": (me + step) % count},
        )

    def send_vec(step, carry):
        vec_copy(step).start()
        return carry

    lax.fori_loop(1, count, send_vec, 0)

    def handle_side(step):
        shard = shard_a(step)
        for k in kinds:
            taken = piece(k, shard, "x")
            remote(taken, taken, side_s.at[k, step], side_r.at[k, step], across).wait_recv()
            core_copy(k, step, shard, "x").start()

    def body(step, is_first, is_last):
        come_a, come_b = shard_a(step), shard_b(step)
        for k in kinds:
            ring_a(k, step, come_a).wait_recv()
            if not is_last:
                ring_a(k, step + 1, come_a).start()
            side_a(k, step, come_a).start()
            core_copy(k, step, come_a, "a").start()
            ring_b(k, step, come_b).wait_recv()
            if not is_last:
                ring_b(k, step + 1, come_b).start()
            core_copy(k, step, come_b, "b").start()
        if not is_first:
            handle_side(step - 1)

    def middle(step, carry):
        body(step, False, False)
        return carry

    body(0, True, False)
    lax.fori_loop(1, count - 2, middle, 0)
    body(count - 2, False, True)
    handle_side(count - 2)

    def finish(step, carry):
        come_a, come_b = shard_a(step), shard_b(step)
        for k in kinds:
            ring_a(k, step, come_a).wait_send()
            ring_b(k, step, come_b).wait_send()
            side_a(k, step, come_a).wait_send()
            for region, shard in (("a", come_a), ("b", come_b), ("x", come_a)):
                copy = core_copy(k, step, shard, region)
                copy.wait_send()
                copy.wait_recv()
        return carry

    lax.fori_loop(0, count - 1, finish, 0)

    def finish_vec(step, carry):
        vec_copy(step).wait_send()
        vec_copy(step).wait_recv()
        return carry

    lax.fori_loop(1, count, finish_vec, 0)
    for copy in own_copies:
        copy.wait()


def gather_weights(w_in, w_out, packed, count):
    in_rows, out_rows, width = w_in.shape[0], w_out.shape[0], w_out.shape[1]
    streams = streams_of(in_rows, out_rows, width)
    kinds, steps = len(streams), count - 1
    dma = pltpu.SemaphoreType.DMA
    return pl.pallas_call(
        functools.partial(gather_kernel, count, streams),
        out_shape=[
            jax.ShapeDtypeStruct((count * in_rows, 3 * width), jnp.bfloat16),
            jax.ShapeDtypeStruct((count * in_rows, 4 * width), jnp.bfloat16),
            jax.ShapeDtypeStruct((count * out_rows, width), jnp.bfloat16),
            jax.ShapeDtypeStruct((count,) + packed.shape, jnp.bfloat16),
        ],
        in_specs=[pl.BlockSpec(memory_space=pltpu.VMEM)] * 3,
        out_specs=[pl.BlockSpec(memory_space=pl.ANY)] * 4,
        scratch_shapes=[dma((kinds, steps))] * 12 + [dma((count,)), dma((count,)), dma((kinds + 1,))],
        compiler_params=pltpu.CompilerParams(collective_id=0, has_side_effects=True),
        name="gather_weights",
    )(w_in, w_out, packed)


def add_into(target, sources):
    rows = target.shape[0]
    block = 16

    def add(index, carry):
        at = pl.ds(pl.multiple_of(index * block, block), block)
        total = target[at, :].astype(jnp.float32)
        for source in sources:
            total = total + source[at, :].astype(jnp.float32)
        target[at, :] = total.astype(jnp.bfloat16)
        return carry

    lax.fori_loop(0, rows // block, add, 0)


def reduce_kernel(count, streams, *refs):
    kinds = range(len(streams))
    kind_count = len(streams)
    given, vec_ref = refs[:3], refs[3]
    final, vec_out = refs[4:7], refs[7]
    refs = refs[8:]
    mine = {r: refs[kind_count * n : kind_count * (n + 1)] for n, r in enumerate("abx")}
    refs = refs[3 * kind_count :]
    other = {r: refs[kind_count * n : kind_count * (n + 1)] for n, r in enumerate("abx")}
    refs = refs[3 * kind_count :]
    from_side, from_a, from_b, last_b, end_b = (
        refs[kind_count * n : kind_count * (n + 1)] for n in range(5)
    )
    refs = refs[5 * kind_count :]
    vec_mine, vec_come, vec_all = refs[:3]
    load, core_s, core_r = refs[3:6]
    side_s, side_r, ring_a_s, ring_a_r, ring_b_s, ring_b_r = refs[6:12]
    end_s, end_r, put = refs[12:15]
    vec_s, vec_r, vec_gs, vec_gr, vec_own = refs[15:]
    group, me, core, side, position, after, before, across, partner = places(count)

    def target_of(step, region):
        if region == "b":
            return ring_shard((position + 1 + step) % count, count)
        return ring_shard((position + 2 * count - 1 - step) % count, count)

    def given_piece(k, step, region, half):
        row = target_of(step, region) * streams[k].rows
        return streams[k].piece(given[k], row, half, side, region)

    def load_copy(k, step, region):
        number = "abx".index(region)
        return pltpu.make_async_copy(
            given_piece(k, step, region, core), mine[region][k].at[step], load.at[number, k, step]
        )

    def core_copy(k, step, region):
        number = "abx".index(region)
        return remote(
            given_piece(k, step, region, 1 - core),
            other[region][k].at[step],
            core_s.at[number, k, step],
            core_r.at[number, k, step],
            partner,
        )

    def begin_load(step, carry):
        for region in "xba":
            for k in kinds:
                load_copy(k, step, region).start()
        return carry

    def begin_core(step, carry):
        for region in "xba":
            for k in kinds:
                core_copy(k, step, region).start()
        return carry

    vec_load = pltpu.make_async_copy(vec_ref.at[me], vec_mine, vec_own.at[0])
    vec_load.start()
    lax.fori_loop(0, count, begin_load, 0)
    greet(me, count, (across, partner, {"grp": (1 - side) * 2 + 1 - core}))
    lax.fori_loop(0, count, begin_core, 0)

    def vec_copy(step):
        to = (me + step) % count
        return remote(
            vec_ref.at[to], vec_come.at[step], vec_s.at[step], vec_r.at[step], {"shard": to}
        )

    def send_vec(step, carry):
        vec_copy(step).start()
        return carry

    lax.fori_loop(1, count, send_vec, 0)

    def side_copy(k, step):
        return remote(
            mine["x"][k].at[step],
            from_side[k].at[step],
            side_s.at[k, step],
            side_r.at[k, step],
            across,
        )

    def ring_a(k, step):
        return remote(
            mine["a"][k].at[step],
            from_a[k].at[step],
            ring_a_s.at[k, step],
            ring_a_r.at[k, step],
            after,
        )

    def ring_b(k, step):
        return remote(
            mine["b"][k].at[step],
            from_b[k].at[step],
            ring_b_s.at[k, step],
            ring_b_r.at[k, step],
            before,
        )

    def ready(k, step, region):
        load_copy(k, step, region).wait()
        core_copy(k, step, region).wait_recv()

    def give_side(step):
        for k in kinds:
            ready(k, step, "x")
            add_into(mine["x"][k].at[step], [other["x"][k].at[step]])
            side_copy(k, step).start()

    def body(step, is_first, is_last):
        for k in kinds:
            ready(k, step, "b")
            terms = [other["b"][k].at[step]]
            if not is_first:
                ring_b(k, step - 1).wait_recv()
                terms.append(from_b[k].at[step - 1])
            add_into(mine["b"][k].at[step], terms)
            if not is_last:
                ring_b(k, step).start()
            ready(k, step, "a")
            side_copy(k, step).wait_recv()
            terms = [other["a"][k].at[step], from_side[k].at[step]]
            if not is_first:
                ring_a(k, step - 1).wait_recv()
                terms.append(from_a[k].at[step - 1])
            add_into(mine["a"][k].at[step], terms)
            if not is_last:
                ring_a(k, step).start()
        if not is_last:
            give_side_next(step)

    def give_side_next(step):
        @pl.when(step + 2 < count)
        def _():
            give_side(step + 2)

    def middle(step, carry):
        body(step, False, False)
        return carry

    give_side(0)
    give_side(1)
    body(0, True, False)
    lax.fori_loop(1, count - 1, middle, 0)
    body(count - 1, False, True)

    last = count - 1

    def final_piece(k, region):
        return streams[k].piece(final[k], 0, core, side, region)

    def end_swap(k):
        return remote(mine["b"][k].at[last], last_b[k], end_s.at[0, k], end_r.at[0, k], across)

    def end_side(k):
        place = final_piece(k, "a")
        return remote(mine["a"][k].at[last], place, end_s.at[1, k], end_r.at[1, k], across)

    def end_core(k, number, region, source):
        place = final_piece(k, region)
        return remote(source, place, end_s.at[number, k], end_r.at[number, k], partner)

    for k in kinds:
        end_swap(k).start()
        end_side(k).start()
    puts = []
    cores = []
    for k in kinds:
        puts.append(
            pltpu.make_async_copy(mine["a"][k].at[last], final_piece(k, "a"), put.at[0, k])
        )
        cores.append(end_core(k, 2, "a", mine["a"][k].at[last]))
        puts[-1].start()
        cores[-1].start()

    def vec_wait(step, carry):
        vec_copy(step).wait_recv()
        return carry

    lax.fori_loop(1, count, vec_wait, 0)
    vec_load.wait()
    vec_come[0] = vec_mine[...]
    total = vec_come[me % count]
    for shard in range(1, count):
        total = total + vec_come[(me + count - shard) % count]
    vec_mine[...] = total
    vec_keep = pltpu.make_async_copy(vec_mine, vec_all.at[group], vec_own.at[1])
    vec_keep.start()

    def vec_group(step):
        return remote(
            vec_mine,
            vec_all.at[group],
            vec_gs.at[step],
            vec_gr.at[step],
            {"grp": (group + step) % 4},
        )

    for step in range(1, 4):
        vec_group(step).start()

    for k in kinds:
        end_swap(k).wait_recv()
        rows = last_b[k].shape[0]

        def add(index, carry, k=k):
            at = pl.ds(pl.multiple_of(index * 16, 16), 16)
            both = mine["b"][k][last, at, :].astype(jnp.float32) + last_b[k][at, :].astype(
                jnp.float32
            )
            end_b[k][at, :] = both.astype(jnp.bfloat16)
            return carry

        lax.fori_loop(0, rows // 16, add, 0)
        puts.append(pltpu.make_async_copy(end_b[k], final_piece(k, "b"), put.at[1, k]))
        cores.append(end_core(k, 3, "b", end_b[k]))
        puts[-1].start()
        cores[-1].start()
        place = final_piece(k, "x")
        remote(place, place, end_s.at[1, k], end_r.at[1, k], across).wait_recv()
        cores.append(end_core(k, 4, "x", place))
        cores[-1].start()

    vec_keep.wait()
    for step in range(1, 4):
        vec_group(step).wait_recv()
    vec_out[...] = vec_all[0] + vec_all[1] + vec_all[2] + vec_all[3]
    for step in range(1, 4):
        vec_group(step).wait_send()

    def finish_vec(step, carry):
        vec_copy(step).wait_send()
        return carry

    lax.fori_loop(1, count, finish_vec, 0)

    def finish_core(step, carry):
        for k in kinds:
            for region in "xba":
                core_copy(k, step, region).wait_send()
            side_copy(k, step).wait_send()
        return carry

    lax.fori_loop(0, count, finish_core, 0)

    def finish_ring(step, carry):
        for k in kinds:
            ring_a(k, step).wait_send()
            ring_b(k, step).wait_send()
        return carry

    lax.fori_loop(0, count - 1, finish_ring, 0)
    for k in kinds:
        end_swap(k).wait_send()
        end_side(k).wait_send()
    for copy in puts:
        copy.wait()
    for copy in cores:
        copy.wait_send()
        copy.wait_recv()


def reduce_grads(grad_qkv, grad_hidden, grad_out, grad_vec, count):
    width = grad_out.shape[1]
    in_rows, out_rows = grad_qkv.shape[0] // count, grad_out.shape[0] // count
    streams = streams_of(in_rows, out_rows, width)
    kinds = len(streams)
    dma = pltpu.SemaphoreType.DMA

    def slots(number, region):
        return [pltpu.VMEM((number,) + s.shape(region), jnp.bfloat16) for s in streams]

    slab = grad_vec.shape[1:]
    return pl.pallas_call(
        functools.partial(reduce_kernel, count, streams),
        out_shape=[
            jax.ShapeDtypeStruct((in_rows, 3 * width), jnp.bfloat16),
            jax.ShapeDtypeStruct((in_rows, 4 * width), jnp.bfloat16),
            jax.ShapeDtypeStruct((out_rows, width), jnp.bfloat16),
            jax.ShapeDtypeStruct(slab, jnp.float32),
        ],
        in_specs=[pl.BlockSpec(memory_space=pl.ANY)] * 4,
        out_specs=[pl.BlockSpec(memory_space=pl.ANY)] * 3
        + [pl.BlockSpec(memory_space=pltpu.VMEM)],
        scratch_shapes=slots(count, "a")
        + slots(count, "b")
        + slots(count, "x")
        + slots(count, "a")
        + slots(count, "b")
        + slots(count, "x")
        + slots(count, "a")
        + slots(count - 1, "a")
        + slots(count - 1, "b")
        + [pltpu.VMEM(s.shape("b"), jnp.bfloat16) for s in streams] * 2
        + [
            pltpu.VMEM(slab, jnp.float32),
            pltpu.VMEM((count,) + slab, jnp.float32),
            pltpu.VMEM((4,) + slab, jnp.float32),
            dma((3, kinds, count)),
            dma((3, kinds, count)),
            dma((3, kinds, count)),
            dma((kinds, count)),
            dma((kinds, count)),
            dma((kinds, count)),
            dma((kinds, count)),
            dma((kinds, count)),
            dma((kinds, count)),
            dma((5, kinds)),
            dma((5, kinds)),
            dma((2, kinds)),
            dma((count,)),
            dma((count,)),
            dma((4,)),
            dma((4,)),
            dma((2,)),
        ],
        compiler_params=pltpu.CompilerParams(
            collective_id=1, has_side_effects=True, vmem_limit_bytes=60000000
        ),
        name="reduce_grads",
    )(grad_qkv, grad_hidden, grad_out, grad_vec)


def turn(values, cosine, low, high, sign):
    size = values.shape[1]
    return (
        values * cosine
        + sign * (pltpu.roll(values, size - ROT // 2, 1) * low + pltpu.roll(values, ROT // 2, 1) * high)
    )


def dot_tt(left, right):
    return lax.dot_general(
        left, right, (((1,), (1,)), ((), ())), preferred_element_type=jnp.float32
    )


def dot_nn(left, right):
    return jnp.dot(left, right, preferred_element_type=jnp.float32)


def attention_block(q_all, k_all, v_all, do_all, bias_ref, out_ref, dq_ref, dk_ref, dv_ref, tables):
    slots = q_all.shape[0]
    tile = min(256, slots)
    pair = 2 * HEAD
    cosine, low, high = tables
    lane = lax.broadcasted_iota(jnp.int32, (slots, pair), 1)
    low_half = lane < HEAD
    for number in range(q_all.shape[1] // pair):
        at = slice(number * pair, (number + 1) * pair)
        query, keys, values, d_out = q_all[:, at], k_all[:, at], v_all[:, at], do_all[:, at]
        keys_t, values_t = keys.T, values.T
        results = []
        for head in range(2):
            own = low_half if head == 0 else jnp.logical_not(low_half)
            zero = jnp.zeros_like(query)
            query_h = jnp.where(own, query, zero)
            d_out_h = jnp.where(own, d_out, zero)
            attended, d_query = [], []
            d_keys = [None] * (slots // tile)
            d_values = [None] * (slots // tile)
            for block in range(slots // tile):
                rows = slice(block * tile, (block + 1) * tile)
                stop = (block + 1) * tile
                scores = dot_tt(keys[:stop], query_h[rows]) + bias_ref[:stop, rows]
                expo = jnp.exp(scores - jnp.max(scores, axis=0, keepdims=True))
                probs = expo * (1.0 / jnp.sum(expo, axis=0, keepdims=True))
                low_probs = probs.astype(jnp.bfloat16)
                attended.append(dot_nn(values_t[:, :stop], low_probs))
                d_probs = dot_tt(values[:stop], d_out_h[rows])
                weighted = jnp.sum(probs * d_probs, axis=0, keepdims=True)
                d_scores = (probs * (d_probs - weighted)).astype(jnp.bfloat16)
                d_query.append(dot_nn(keys_t[:, :stop], d_scores))
                part_k = dot_nn(d_scores, query[rows])
                part_v = dot_nn(low_probs, d_out[rows])
                for piece in range(block + 1):
                    cut = slice(piece * tile, (piece + 1) * tile)
                    if d_keys[piece] is None:
                        d_keys[piece], d_values[piece] = part_k[cut], part_v[cut]
                    else:
                        d_keys[piece] = d_keys[piece] + part_k[cut]
                        d_values[piece] = d_values[piece] + part_v[cut]
            results.append(
                (
                    jnp.concatenate(attended, axis=1),
                    jnp.concatenate(d_query, axis=1),
                    jnp.concatenate(d_keys, axis=0),
                    jnp.concatenate(d_values, axis=0),
                )
            )
        first, second = results
        top = lax.broadcasted_iota(jnp.int32, (pair, slots), 0) < HEAD
        out_ref[:, at] = jnp.where(top, first[0], second[0]).T.astype(jnp.bfloat16)
        d_query = jnp.where(top, first[1], second[1]).T * (HEAD**-0.5)
        dq_ref[:, at] = turn(d_query, cosine, low, high, -1.0).astype(jnp.bfloat16)
        d_keys = jnp.where(low_half, first[2], second[2])
        dk_ref[:, at] = turn(d_keys, cosine, low, high, -1.0).astype(jnp.bfloat16)
        dv_ref[:, at] = jnp.where(low_half, first[3], second[3]).astype(jnp.bfloat16)


def attention_kernel(
    a_ref, dy_ref, wq_ref, wk_ref, wv_ref, bq_ref, bk_ref, bv_ref, wo_ref, cos_ref, low_ref,
    high_ref, row_ref, col_ref, out_ref, dq_ref, dk_ref, dv_ref, bias_ref
):
    slots = a_ref.shape[0]

    @pl.when(pl.program_id(0) == 0)
    def _():
        key = lax.broadcasted_iota(jnp.int32, (slots, slots), 0)
        query = lax.broadcasted_iota(jnp.int32, (slots, slots), 1)
        allowed = (key <= query) & (col_ref[...] == row_ref[...])
        bias_ref[...] = jnp.where(allowed, 0.0, NEG)

    tables = (cos_ref[...], low_ref[...], high_ref[...])
    pair = 2 * HEAD

    def project(w_ref, b_ref, scale):
        flat = dot_nn(a_ref[...], w_ref[...]) + b_ref[...]
        if scale is None:
            return flat.astype(jnp.bfloat16)
        parts = [
            (turn(flat[:, i : i + pair], *tables, 1.0)).astype(jnp.bfloat16) * scale
            for i in range(0, flat.shape[1], pair)
        ]
        return jnp.concatenate(parts, axis=1)

    query = project(wq_ref, bq_ref, jnp.bfloat16(HEAD**-0.5))
    keys = project(wk_ref, bk_ref, jnp.bfloat16(1.0))
    values = project(wv_ref, bv_ref, None)
    d_out = dot_tt(dy_ref[...], wo_ref[...]).astype(jnp.bfloat16)
    attention_block(
        query, keys, values, d_out, bias_ref, out_ref, dq_ref, dk_ref, dv_ref, tables
    )


def rotary_lanes(doc_ids):
    cosine, sine = rotary_tables(doc_ids)
    slots, half = cosine.shape[0], ROT // 2
    rest = jnp.zeros((slots, HEAD - ROT), jnp.float32)
    blank = jnp.zeros((slots, half), jnp.float32)
    cos_lanes = jnp.concatenate([cosine, rest + 1.0], axis=1)
    low = jnp.concatenate([-sine[:, :half], blank, rest], axis=1)
    high = jnp.concatenate([blank, sine[:, half:], rest], axis=1)
    return tuple(jnp.concatenate([t, t], axis=1) for t in (cos_lanes, low, high))


def attention(normed, d_out_low, w_qkv, bias_qkv, w_out, doc_ids):
    slots, width = normed.shape
    group = 4 * HEAD
    parts = width // group
    whole = lambda shape: pl.BlockSpec(shape, lambda i: (0, 0))
    column = lambda rows, n: pl.BlockSpec((rows, group), lambda i: (0, n * parts + i))
    result = pl.BlockSpec((slots, group), lambda i: (0, i))
    bias = bias_qkv.reshape(1, 3 * width)
    return pl.pallas_call(
        attention_kernel,
        grid=(parts,),
        out_shape=[jax.ShapeDtypeStruct((slots, width), jnp.bfloat16)] * 4,
        in_specs=[whole((slots, width)), whole((slots, width))]
        + [column(width, n) for n in range(3)]
        + [column(1, n) for n in range(3)]
        + [pl.BlockSpec((group, width), lambda i: (i, 0))]
        + [whole((slots, 2 * HEAD))] * 3
        + [whole((1, slots)), whole((slots, 1))],
        out_specs=[result] * 4,
        scratch_shapes=[pltpu.VMEM((slots, slots), jnp.float32)],
        compiler_params=pltpu.CompilerParams(vmem_limit_bytes=50000000),
        name="attention",
    )(
        normed, d_out_low, w_qkv, w_qkv, w_qkv, bias, bias, bias, w_out, *rotary_lanes(doc_ids),
        doc_ids.reshape(1, slots), doc_ids.reshape(slots, 1),
    )


def shards(
    count,
    inputs,
    cotangent,
    doc_ids,
    master_in,
    master_out,
    vectors,
    moment_in,
    moment_out,
    moment_vec,
    square_in,
    square_out,
    square_vec,
):
    slots, width = inputs.shape
    live = (doc_ids < SEQ_DEV).astype(jnp.float32)[:, None]
    w_qkv, w_hidden, w_out, packed = gather_weights(
        master_in.astype(jnp.bfloat16),
        master_out.astype(jnp.bfloat16),
        jnp.pad(vectors, ((0, 4), (0, 0))).astype(jnp.bfloat16),
        count,
    )
    packed = packed.transpose(1, 0, 2).reshape(16, width)
    (
        first_norm_gain,
        first_norm_offset,
        second_norm_gain,
        second_norm_offset,
        bias_qkv,
        bias_hidden,
        bias_out,
    ) = unpack(packed, width)
    residual_stream = inputs.astype(jnp.float32)
    branch_input_first, first_normalized, first_inverse_deviation = layer_norm_apply(
        residual_stream, first_norm_gain, first_norm_offset
    )
    branch_input_second, second_normalized, second_inverse_deviation = layer_norm_apply(
        residual_stream, second_norm_gain, second_norm_offset
    )
    branch_input_first = branch_input_first.astype(jnp.bfloat16)
    branch_input_second = branch_input_second.astype(jnp.bfloat16)
    hidden = (
        jnp.dot(branch_input_second, w_hidden, preferred_element_type=jnp.float32)
        + bias_hidden
    )
    d_out = cotangent.astype(jnp.float32) * live
    d_out_low = d_out.astype(jnp.bfloat16)
    attended, d_query, d_keys, d_values = attention(
        branch_input_first, d_out_low, w_qkv, bias_qkv, w_out, doc_ids
    )
    active = gelu_value(hidden).astype(jnp.bfloat16)
    joined = jnp.concatenate([attended, active], axis=1)
    branch = jnp.dot(joined, w_out, preferred_element_type=jnp.float32) + bias_out
    output = ((residual_stream + branch) * live).astype(jnp.bfloat16)
    d_active = contract_cols(d_out_low, w_out[width:])
    grad_out_term = contract_rows(joined, d_out_low)
    d_hidden = (d_active * gelu_slope(hidden)).astype(jnp.bfloat16)
    d_qkv = jnp.concatenate([d_query, d_keys, d_values], axis=1)
    grad_qkv_term = contract_rows(branch_input_first, d_qkv)
    grad_hidden_term = contract_rows(branch_input_second, d_hidden)
    gradient_branch_first = contract_cols(d_qkv, w_qkv)
    gradient_branch_second = contract_cols(d_hidden, w_hidden)
    gradient_stream_first, gradient_gain_first, gradient_offset_first = layer_norm_gradient(
        gradient_branch_first, first_normalized, first_inverse_deviation, first_norm_gain
    )
    gradient_stream_second, gradient_gain_second, gradient_offset_second = layer_norm_gradient(
        gradient_branch_second, second_normalized, second_inverse_deviation, second_norm_gain
    )
    input_grad = d_out + gradient_stream_first + gradient_stream_second
    grad_vec_term = jnp.concatenate(
        [
            gradient_gain_first[None],
            gradient_offset_first[None],
            gradient_gain_second[None],
            gradient_offset_second[None],
            jnp.sum(d_qkv, axis=0, dtype=jnp.float32).reshape(3, width),
            jnp.sum(d_hidden, axis=0, dtype=jnp.float32).reshape(4, width),
            jnp.sum(d_out, axis=0)[None],
        ],
        axis=0,
    )
    vec_slabs = jnp.pad(grad_vec_term, ((0, 4), (0, 0)))
    vec_slabs = vec_slabs.reshape(16, count, width // count).transpose(1, 0, 2)
    sum_qkv, sum_hidden, sum_out, sum_vec = reduce_grads(
        grad_qkv_term.astype(jnp.bfloat16),
        grad_hidden_term.astype(jnp.bfloat16),
        grad_out_term.astype(jnp.bfloat16),
        vec_slabs,
        count,
    )
    grad_in = jnp.concatenate([sum_qkv, sum_hidden], axis=1).astype(jnp.float32)
    grad_out = sum_out.astype(jnp.float32)
    grad_vec = sum_vec[:12]
    update_in, moment_in_next, square_in_next = adam(master_in, moment_in, square_in, grad_in, 0.1)
    update_out, moment_out_next, square_out_next = adam(
        master_out, moment_out, square_out, grad_out, 0.1
    )
    update_vec, moment_vec_next, square_vec_next = adam(
        vectors, moment_vec, square_vec, grad_vec, 0.0
    )
    return (
        output,
        input_grad,
        grad_in,
        grad_out,
        grad_vec,
        update_in,
        update_out,
        update_vec,
        moment_in_next,
        moment_out_next,
        moment_vec_next,
        square_in_next,
        square_out_next,
        square_vec_next,
    )


def solution(mesh):
    placed = (
        P(("grp", "shard"), None),
        P(("grp", "shard"), None),
        P(("grp", "shard")),
        P("shard", None),
        P("shard", None),
        P(None, "shard"),
        P("shard", None),
        P("shard", None),
        P(None, "shard"),
        P("shard", None),
        P("shard", None),
        P(None, "shard"),
    )
    return jax.shard_map(
        functools.partial(shards, mesh.shape["shard"]),
        mesh=mesh,
        in_specs=placed,
        out_specs=(
            P(("grp", "shard"), None),
            P(("grp", "shard"), None),
            P("shard", None),
            P("shard", None),
            P(None, "shard"),
            P("shard", None),
            P("shard", None),
            P(None, "shard"),
            P("shard", None),
            P("shard", None),
            P(None, "shard"),
            P("shard", None),
            P("shard", None),
            P(None, "shard"),
        ),
        check_vma=False,
    )
```
